32 devices in a mesh: groups: 2 (over x), steps: 8 (over z, y), inner: 2 (over core).
Axes of the slice: x: 2, y: 2, z: 4, core: 2. Of those that a mesh axis runs over, the one named last changes fastest.
Arguments:
- start_state: float32 [16, 32, 768], P('groups'), parts along dimension 0, may hold values from -6 to 6
- noise_draws: float32 [32, 8, 32, 768], P(('groups', 'steps', 'inner')), parts along dimension 0, may hold values from -6 to 6
- step_gaps: int32 [32], P(('groups', 'steps', 'inner')), parts along dimension 0, may hold values from 1 to 15
- window_start: int32 [2], P('groups'), parts along dimension 0, may hold values from 240 to 999
- input_weight: bfloat16 [768, 1024], replicated, may hold values from -0.21875 to 0.21875
- embed_weight: bfloat16 [256, 2048], replicated, may hold values from -0.375 to 0.375
- first_weight: bfloat16 [1024, 1024], replicated, may hold values from -0.1875 to 0.1875
- second_weight: bfloat16 [1024, 1024], replicated, may hold values from -0.1875 to 0.1875
- output_weight: bfloat16 [1024, 768], replicated, may hold values from -0.1875 to 0.1875
Outputs:
- trajectory: float32 [32, 8, 32, 768], P(('groups', 'steps', 'inner')), parts along dimension 0
The draws below stay inside these ranges and needn't reach their ends.
There are 2 independent parts, one for each index of `groups`. The reference program is written for one: setup_inputs(seed, part) draws one part's arguments, and reference() takes and returns one part's arrays. A program takes and returns all parts, laid end to end along the dimension named above; an argument that names none is the same for every part. Nothing has to cross between parts.
All inputs are finite; a program needn't handle non-finite values.
Results may differ from the reference program's by a relative error of at most 0.00035.
Values sent between devices are 32-bit elements; how exact they have to be, the bound alone decides.
No kernel may reach another device: no remote copies, remote signals or barrier semaphores. Data moves between devices by JAX's collectives and lax.ppermute only.
A program may use at most 64 MiB of HBM per device.

```python
import math
import jax
import jax.numpy as jnp
from jax import lax

BATCH = 8
PATCHES = 32
FEATURES = 768
CHANNELS = 1024
FREQS = 128
GROUPS = 32
ITERS = 2
GAP_MAX = 15
TRAIN_STEPS = 1000
WINDOW = 16


def place_ends(array, rng, low, high):
    place = [jax.random.randint(jax.random.fold_in(rng, axis), (), 0, length) for axis, length in enumerate(array.shape)]
    main_axis = array.shape.index(max(array.shape))
    neighbour = place[:main_axis] + [(place[main_axis] + 1) % array.shape[main_axis]] + place[main_axis + 1:]
    return array.at[tuple(place)].set(low).at[tuple(neighbour)].set(high)


def shard_levels(stream_key, dims, split, least, largest):
    def one(position, shards_of):
        heights = jax.random.uniform(jax.random.fold_in(jax.random.fold_in(stream_key, 6), position), (shards_of,), jnp.float32, least / len(split), largest / len(split))
        return jnp.repeat(jnp.exp(heights), dims[position] // shards_of).reshape((-1,) + (1,) * (len(dims) - position - 1))

    level = one(*split[0])
    for cut in split[1:]:
        level = level * one(*cut)
    return level


def scatter_about(own_key, shape, deviation, bound, cuts=(), held_as=jnp.bfloat16):
    drawn = deviation * jax.random.normal(own_key, shape, jnp.float32)
    if cuts:
        drawn = drawn * shard_levels(own_key, shape, cuts, -0.22, 0.18)
    return jnp.clip(drawn, -bound, bound).astype(held_as)


def setup_inputs(seed: int = 0, part: int = 0) -> dict:
    key_list = jax.random.split(jax.random.key(seed), 10)
    part_keys = jax.random.split(jax.random.fold_in(key_list[9], part), 10)
    start_state = scatter_about(part_keys[0], (BATCH, PATCHES, FEATURES), 1.0, 6.0, (), jnp.float32)
    noise_draws = scatter_about(part_keys[1], (WINDOW, BATCH, PATCHES, FEATURES), 1.0, 6.0, ((0, 16),), jnp.float32)
    step_gaps = place_ends(jax.random.randint(part_keys[2], (WINDOW,), 1, GAP_MAX + 1), jax.random.fold_in(part_keys[2], 1), 1, GAP_MAX).astype(jnp.int32)
    window_start = jax.random.randint(part_keys[3], (1,), WINDOW * GAP_MAX, TRAIN_STEPS).astype(jnp.int32)
    input_weight = scatter_about(key_list[4], (FEATURES, CHANNELS), FEATURES ** -0.5, 0.21875)
    embed_weight = scatter_about(key_list[5], (2 * FREQS, 2 * CHANNELS), (2 * FREQS) ** -0.5, 0.375)
    first_weight = scatter_about(key_list[6], (CHANNELS, CHANNELS), CHANNELS ** -0.5, 0.1875)
    second_weight = scatter_about(key_list[7], (CHANNELS, CHANNELS), CHANNELS ** -0.5, 0.1875)
    output_weight = scatter_about(key_list[8], (CHANNELS, FEATURES), CHANNELS ** -0.5, 0.1875)
    return dict(start_state=start_state, noise_draws=noise_draws, step_gaps=step_gaps, window_start=window_start, input_weight=input_weight, embed_weight=embed_weight, first_weight=first_weight, second_weight=second_weight, output_weight=output_weight)


def noise_table():
    levels = jnp.arange(TRAIN_STEPS, dtype=jnp.float32)
    beta_values = 0.0001 + (0.02 - 0.0001) * levels / (TRAIN_STEPS - 1)
    return jnp.exp(jnp.cumsum(jnp.log1p(-beta_values)))

def lookup(table, noise_level):
    places = jnp.arange(TRAIN_STEPS, dtype=jnp.int32)
    return jnp.sum(jnp.where(places == noise_level, table, jnp.zeros_like(table)))

def group_norm(hidden, batch_count):
    total_rows, channel_count = hidden.shape
    shaped = hidden.reshape(batch_count, total_rows // batch_count, channel_count)

    def group_mean(values):
        per_channel = lax.optimization_barrier(jnp.mean(values, axis=1)).reshape(batch_count, GROUPS, channel_count // GROUPS)
        per_group = lax.optimization_barrier(jnp.mean(per_channel, axis=2, keepdims=True))
        return jnp.broadcast_to(per_group, per_channel.shape).reshape(batch_count, 1, channel_count)
    center = group_mean(shaped)
    offset = shaped - center
    spread = group_mean(offset * offset)
    return (offset * lax.rsqrt(spread + 1e-05)).reshape(total_rows, channel_count)

def predict_noise(state, noise_level, input_weight, embed_weight, first_weight, second_weight, output_weight):
    batch_count, patch_count, feature_count = state.shape
    channel_count = input_weight.shape[1]
    flat_state = state.reshape(batch_count * patch_count, feature_count).astype(jnp.bfloat16)
    entry_hidden = jnp.dot(flat_state, input_weight, preferred_element_type=jnp.float32)
    half_count = embed_weight.shape[0] // 2
    frequency = jnp.exp(-math.log(10000.0) * jnp.arange(half_count, dtype=jnp.float32) / half_count)
    angles = noise_level.astype(jnp.float32) * frequency
    features = jnp.concatenate([jnp.cos(angles), jnp.sin(angles)])[None, :].astype(jnp.bfloat16)
    modulation = jnp.dot(features, embed_weight, preferred_element_type=jnp.float32)
    scale_part = modulation[:, :channel_count]
    shift_part = modulation[:, channel_count:]
    act_one = jax.nn.silu(group_norm(entry_hidden, batch_count) * (1.0 + scale_part) + shift_part).astype(jnp.bfloat16)
    middle = jnp.dot(act_one, first_weight, preferred_element_type=jnp.float32)
    act_two = jax.nn.silu(group_norm(middle, batch_count)).astype(jnp.bfloat16)
    block_out = entry_hidden + jnp.dot(act_two, second_weight, preferred_element_type=jnp.float32)
    act_three = jax.nn.silu(group_norm(block_out, batch_count)).astype(jnp.bfloat16)
    predicted = jnp.dot(act_three, output_weight, preferred_element_type=jnp.float32)
    return predicted.reshape(state.shape)

def drift_of(state, noise_draw, level_now, level_next, table, input_weight, embed_weight, first_weight, second_weight, output_weight):
    predicted = predict_noise(state, level_now, input_weight, embed_weight, first_weight, second_weight, output_weight)
    bar_now = lookup(table, level_now)
    bar_next = lookup(table, level_next)
    clean_guess = jnp.clip((state - jnp.sqrt(1.0 - bar_now) * predicted) / jnp.sqrt(bar_now), -1.0, 1.0)
    implied = (state - jnp.sqrt(bar_now) * clean_guess) / jnp.sqrt(1.0 - bar_now)
    sigma_value = jnp.sqrt((1.0 - bar_next) / (1.0 - bar_now) * (1.0 - bar_now / bar_next))
    noise_coef = (1.0 - bar_next) * jnp.sqrt(bar_now / (bar_next * (1.0 - bar_now)))
    return jnp.sqrt(bar_next) * clean_guess + noise_coef * implied + sigma_value * noise_draw - state

def reference(start_state, noise_draws, step_gaps, window_start, input_weight, embed_weight, first_weight, second_weight, output_weight):
    table = noise_table()
    before = jnp.cumsum(step_gaps) - step_gaps
    level_now = (window_start[0] - before).astype(jnp.int32)
    level_next = (level_now - step_gaps).astype(jnp.int32)
    states = jnp.broadcast_to(start_state[None], noise_draws.shape)

    def one_step(item):
        return drift_of(item[0], item[1], item[2], item[3], table, input_weight, embed_weight, first_weight, second_weight, output_weight)
    totals = states
    for iteration in range(ITERS):
        drifts = lax.map(one_step, (states, noise_draws, level_now, level_next))
        totals = jnp.cumsum(drifts, axis=0)
        states = start_state[None] + (totals - drifts)
    return start_state[None] + totals
```

```python
import math

import jax
import jax.numpy as jnp
from jax import lax
from jax.sharding import PartitionSpec as P

GROUPS = 32
ITERS = 2
TRAIN_STEPS = 1000
TIME = ("steps", "inner")


def noise_table():
    levels = jnp.arange(TRAIN_STEPS, dtype=jnp.float32)
    beta_values = 0.0001 + (0.02 - 0.0001) * levels / (TRAIN_STEPS - 1)
    return jnp.exp(jnp.cumsum(jnp.log1p(-beta_values)))


def lookup(table, levels):
    places = jnp.arange(TRAIN_STEPS, dtype=jnp.int32)
    return jnp.sum(jnp.where(places == levels[:, None], table, jnp.zeros_like(table)), axis=1)


def group_norm(hidden):
    times, patches, channels = hidden.shape

    def group_mean(values):
        per_channel = jnp.mean(values, axis=1).reshape(times, GROUPS, channels // GROUPS)
        per_group = jnp.mean(per_channel, axis=2, keepdims=True)
        return jnp.broadcast_to(per_group, per_channel.shape).reshape(times, 1, channels)

    offset = hidden - group_mean(hidden)
    return offset * lax.rsqrt(group_mean(offset * offset) + 1e-05)


def project(values, weight):
    return lax.dot_general(
        values.astype(jnp.bfloat16),
        weight,
        (((2,), (0,)), ((), ())),
        preferred_element_type=jnp.float32,
    )


def predict_noise(states, modulation, input_weight, first_weight, second_weight, output_weight):
    channels = input_weight.shape[1]
    scale_part = modulation[:, None, :channels]
    shift_part = modulation[:, None, channels:]
    entry = project(states, input_weight)
    act_one = jax.nn.silu(group_norm(entry) * (1.0 + scale_part) + shift_part)
    act_two = jax.nn.silu(group_norm(project(act_one, first_weight)))
    block = entry + project(act_two, second_weight)
    return project(jax.nn.silu(group_norm(block)), output_weight)


def shift_blocks(part, count, width, blocks):
    pairs = [(place, place + blocks * width) for place in range(count - blocks * width)]
    return lax.ppermute(part, TIME, pairs)


def earlier_blocks(part, count, width):
    total = shift_blocks(part, count, width, 1)
    reach = 1
    while reach < count // width - 1:
        total = total + shift_blocks(total, count, width, reach)
        reach *= 2
    return total


def shards(
    start_state,
    noise_draws,
    step_gaps,
    window_start,
    input_weight,
    embed_weight,
    first_weight,
    second_weight,
    output_weight,
):
    count = lax.axis_size(TIME)
    width = start_state.shape[0]
    assert count % width == 0
    groups = [list(range(first, first + width)) for first in range(0, count, width)]
    place = lax.axis_index(TIME)
    image = place % width
    first_time = place - image

    def exchange(values):
        return lax.all_to_all(values, TIME, 0, 0, axis_index_groups=groups, tiled=True)

    noise = exchange(noise_draws[0])
    later = jnp.arange(count + 1, dtype=jnp.int32) > place
    before = lax.psum(jnp.where(later, step_gaps[0], 0), TIME)
    marks = window_start[0] - lax.dynamic_slice_in_dim(before, first_time, width + 1)
    bars = lookup(noise_table(), marks)
    bar_now = bars[:-1, None, None]
    bar_next = bars[1:, None, None]
    half = embed_weight.shape[0] // 2
    frequency = jnp.exp(-math.log(10000.0) * jnp.arange(half, dtype=jnp.float32) / half)
    angles = marks[:-1, None].astype(jnp.float32) * frequency
    features = jnp.concatenate([jnp.cos(angles), jnp.sin(angles)], axis=1).astype(jnp.bfloat16)
    modulation = jnp.dot(features, embed_weight, preferred_element_type=jnp.float32)
    sigma = jnp.sqrt((1.0 - bar_next) / (1.0 - bar_now) * (1.0 - bar_now / bar_next))
    noise_coef = (1.0 - bar_next) * jnp.sqrt(bar_now / (bar_next * (1.0 - bar_now)))

    own = lax.dynamic_index_in_dim(start_state, image, 0, True)
    states = own
    for iteration in range(ITERS):
        predicted = predict_noise(
            states, modulation, input_weight, first_weight, second_weight, output_weight
        )
        clean = jnp.clip(
            (states - jnp.sqrt(1.0 - bar_now) * predicted) / jnp.sqrt(bar_now), -1.0, 1.0
        )
        implied = (states - jnp.sqrt(bar_now) * clean) / jnp.sqrt(1.0 - bar_now)
        drift = jnp.sqrt(bar_next) * clean + noise_coef * implied + sigma * noise - states
        totals = jnp.cumsum(drift, axis=0)
        base = own + earlier_blocks(totals[-1:], count, width)
        states = base + (totals - drift)
    return exchange(states + drift)[None]


def solution(mesh):
    return jax.shard_map(
        shards,
        mesh=mesh,
        in_specs=(
            P("groups", None, None),
            P(("groups", "steps", "inner"), None, None, None),
            P(("groups", "steps", "inner")),
            P("groups"),
            P(),
            P(),
            P(),
            P(),
            P(),
        ),
        out_specs=P(("groups", "steps", "inner"), None, None, None),
        check_vma=False,
    )
```

```python
import functools
import math

import jax
import jax.numpy as jnp
import numpy as np
from jax import lax
from jax.experimental import pallas as pl
from jax.experimental.pallas import tpu as pltpu
from jax.sharding import PartitionSpec as P

GROUPS = 32
TRAIN_STEPS = 1000
TIME = ("steps", "inner")
LANES = 128
CHUNK = 256
COEFS = 5


def noise_table():
    levels = np.arange(TRAIN_STEPS, dtype=np.float64)
    betas = 0.0001 + (0.02 - 0.0001) * levels / (TRAIN_STEPS - 1)
    padded = np.zeros((1, -(-TRAIN_STEPS // LANES) * LANES), np.float32)
    padded[0, :TRAIN_STEPS] = np.exp(np.cumsum(np.log1p(-betas)))
    return padded


def group_mean(sums, size, count):
    lane = lax.broadcasted_iota(jnp.int32, sums.shape, 1)
    reach = 1
    while reach < size:
        upper = (lane & reach) != 0
        sums = sums + jnp.where(
            upper, pltpu.roll(sums, reach, 1), pltpu.roll(sums, LANES - reach, 1)
        )
        reach *= 2
    return sums * (1.0 / count)


def norm_silu(hidden_ref, act_ref, first, times, size, scale_ref, shift_ref):
    rows = hidden_ref.shape[0]
    patches = rows // times
    for lane in range(first, first + CHUNK, LANES):
        columns = slice(lane, lane + LANES)
        values = hidden_ref[:, columns].reshape(patches, times, LANES)
        mean = group_mean(jnp.sum(values, axis=0), size, patches * size)
        offset = values - mean
        spread = group_mean(jnp.sum(offset * offset, axis=0), size, patches * size)
        gain = 0.5 * lax.rsqrt(spread + 1e-05)
        if scale_ref is None:
            half = offset * gain
        else:
            gain = gain * (1.0 + scale_ref[:, columns])
            half = offset * gain + 0.5 * shift_ref[:, columns]
        act = half * jnp.tanh(half) + half
        act_ref[:, columns] = act.reshape(rows, LANES).astype(jnp.bfloat16)


def dot(left, right):
    return jnp.dot(left, right, preferred_element_type=jnp.float32)


def network(times, rows_ref, scale_ref, shift_ref, weights, entry_ref, hidden_ref, one_ref, two_ref, eps_ref):
    input_weight, first_weight, second_weight, output_weight = weights
    features, channels = input_weight.shape
    size = channels // GROUPS
    flat = jnp.concatenate([rows_ref[block] for block in range(features // LANES)], axis=1)
    flat = flat.astype(jnp.bfloat16)
    for first in range(0, channels, CHUNK):
        columns = slice(first, first + CHUNK)
        entry_ref[:, columns] = dot(flat, input_weight[:, columns])
        norm_silu(entry_ref, one_ref, first, times, size, scale_ref, shift_ref)
    for first in range(0, channels, CHUNK):
        columns = slice(first, first + CHUNK)
        hidden_ref[:, columns] = dot(one_ref[...], first_weight[:, columns])
        norm_silu(hidden_ref, two_ref, first, times, size, None, None)
    for first in range(0, channels, CHUNK):
        columns = slice(first, first + CHUNK)
        hidden_ref[:, columns] = entry_ref[:, columns] + dot(
            two_ref[...], second_weight[:, columns]
        )
        norm_silu(hidden_ref, one_ref, first, times, size, None, None)
    for first in range(0, features, CHUNK):
        part = dot(one_ref[...], output_weight[:, first : first + CHUNK])
        for lane in range(0, CHUNK, LANES):
            eps_ref[(first + lane) // LANES] = part[:, lane : lane + LANES]


def coefficients(now, later):
    ratio = (1.0 - later) / (1.0 - now)
    keep = ratio * jnp.sqrt(now / later)
    return (
        1.0 / jnp.sqrt(now),
        jnp.sqrt((1.0 - now) / now),
        (later - now) / (jnp.sqrt(later) * (1.0 - now)),
        keep - 1.0,
        jnp.sqrt(ratio * (1.0 - now / later)),
    )


def drift(state, eps, noise, coefs):
    inverse, slope, clean_part, state_part, sigma = coefs
    clean = jnp.clip(inverse * state - slope * eps, -1.0, 1.0)
    return clean_part * clean + state_part * state + sigma * noise


def spread_rows(rows_ref, step, stride, values):
    patches, features = values.shape
    for block in range(features // LANES):
        part = values[:, block * LANES : (block + 1) * LANES]
        rows_ref[block, pl.ds(step, patches, stride), :] = part


def first_kernel(
    width,
    start_ref,
    noise_ref,
    marks_ref,
    table_ref,
    input_ref,
    embed_ref,
    first_ref,
    second_ref,
    output_ref,
    state_ref,
    total_ref,
    scale_ref,
    shift_ref,
    coef_ref,
    own_ref,
    noise_buf,
    rows_ref,
    entry_ref,
    hidden_ref,
    one_ref,
    two_ref,
    eps_ref,
    sems,
):
    place = lax.axis_index(TIME)
    image = lax.rem(place, width)
    own_copy = pltpu.make_async_copy(start_ref.at[image], own_ref, sems.at[0])
    own_copy.start()
    noise_copy = pltpu.make_async_copy(noise_ref, noise_buf, sems.at[1])
    noise_copy.start()

    patches, features = own_ref.shape
    lane = lax.broadcasted_iota(jnp.int32, (width, marks_ref.shape[1]), 1)
    time = lax.broadcasted_iota(jnp.int32, lane.shape, 0)
    marks = marks_ref[...].astype(jnp.float32)
    spot = place - image + time
    now_mark = jnp.sum(jnp.where(lane == spot, marks, 0.0), axis=1, keepdims=True)
    next_mark = jnp.sum(jnp.where(lane == spot + 1, marks, 0.0), axis=1, keepdims=True)
    level = lax.broadcasted_iota(jnp.int32, (width, table_ref.shape[1]), 1).astype(jnp.float32)
    table = table_ref[...]
    now = jnp.sum(jnp.where(level == now_mark, table, 0.0), axis=1, keepdims=True)
    later = jnp.sum(jnp.where(level == next_mark, table, 0.0), axis=1, keepdims=True)
    coefs = coefficients(now, later)
    for index, coef in enumerate(coefs):
        coef_ref[index] = jnp.broadcast_to(coef, (width, LANES))

    half = embed_ref.shape[0] // 2
    order = lax.broadcasted_iota(jnp.int32, (1, half), 1).astype(jnp.float32)
    angles = now_mark * jnp.exp(-math.log(10000.0) * order / half)
    channels = input_ref.shape[1]
    cosine = jnp.cos(angles).astype(jnp.bfloat16)
    sine = jnp.sin(angles).astype(jnp.bfloat16)
    both = jnp.concatenate([cosine, sine], axis=1)
    scale_ref[...] = dot(both, embed_ref[:, :channels])
    shift_ref[...] = dot(both, embed_ref[:, channels:])

    own_copy.wait()
    own = own_ref[...]
    for step in range(width):
        spread_rows(rows_ref, step, width, own)
    weights = (input_ref, first_ref, second_ref, output_ref)
    network(
        width, rows_ref, scale_ref, shift_ref, weights, entry_ref, hidden_ref, one_ref, two_ref, eps_ref
    )
    noise_copy.wait()
    for block in range(features // LANES):
        columns = slice(block * LANES, (block + 1) * LANES)
        base = own_ref[:, columns]
        running = None
        for step in range(width):
            eps = eps_ref[block, pl.ds(step, patches, width), :]
            row = [coef_ref[index, step : step + 1, :] for index in range(COEFS)]
            state_ref[step, :, columns] = base if running is None else base + running
            change = drift(base, eps, noise_buf[step, :, columns], row)
            running = change if running is None else running + change
        total_ref[:, columns] = running


def second_kernel(
    width,
    state_ref,
    earlier_ref,
    noise_ref,
    scale_ref,
    shift_ref,
    coef_ref,
    input_ref,
    first_ref,
    second_ref,
    output_ref,
    sum_ref,
    total_ref,
    noise_buf,
    rows_ref,
    entry_ref,
    hidden_ref,
    one_ref,
    two_ref,
    eps_ref,
    sems,
):
    noise_copy = pltpu.make_async_copy(noise_ref, noise_buf, sems.at[0])
    noise_copy.start()
    patches, features = earlier_ref.shape
    for step in range(width):
        spread_rows(rows_ref, step, width, state_ref[step] + earlier_ref[...])
    weights = (input_ref, first_ref, second_ref, output_ref)
    network(
        width, rows_ref, scale_ref, shift_ref, weights, entry_ref, hidden_ref, one_ref, two_ref, eps_ref
    )
    noise_copy.wait()
    for block in range(features // LANES):
        columns = slice(block * LANES, (block + 1) * LANES)
        own = state_ref[0, :, columns]
        running = None
        for step in range(width):
            eps = eps_ref[block, pl.ds(step, patches, width), :]
            row = [coef_ref[index, step : step + 1, :] for index in range(COEFS)]
            state = state_ref[step, :, columns] + earlier_ref[:, columns]
            change = drift(state, eps, noise_buf[step, :, columns], row)
            running = change if running is None else running + change
            sum_ref[step, :, columns] = own + running
        total_ref[:, columns] = running


def shift_blocks(part, count, width, blocks):
    pairs = [(place, place + blocks * width) for place in range(count - blocks * width)]
    return lax.ppermute(part, TIME, pairs)


def earlier_blocks(part, count, width):
    total = shift_blocks(part, count, width, 1)
    reach = 1
    while reach < count // width - 1:
        total = total + shift_blocks(total, count, width, reach)
        reach *= 2
    return total


def shards(
    start_state,
    noise_draws,
    step_gaps,
    window_start,
    input_weight,
    embed_weight,
    first_weight,
    second_weight,
    output_weight,
):
    count = lax.axis_size(TIME)
    width, patches, features = start_state.shape
    channels = input_weight.shape[1]
    assert count % width == 0 and width % 8 == 0
    groups = [list(range(first, first + width)) for first in range(0, count, width)]
    place = lax.axis_index(TIME)

    def exchange(values):
        return lax.all_to_all(values, TIME, 0, 0, axis_index_groups=groups, tiled=True)

    noise = exchange(noise_draws[0])
    marks_length = -(-(count + 1) // LANES) * LANES
    later = jnp.arange(marks_length, dtype=jnp.int32) > place
    opening = jnp.where(place == 0, window_start[0], 0)
    marks = lax.psum(opening - jnp.where(later, step_gaps[0], 0), TIME)[None]

    def shape(*dims):
        return jax.ShapeDtypeStruct(dims, jnp.float32)

    vmem = pl.BlockSpec(memory_space=pltpu.VMEM)
    anywhere = pl.BlockSpec(memory_space=pl.ANY)
    rows = width * patches
    work = [
        pltpu.VMEM((width, patches, features), jnp.float32),
        pltpu.VMEM((features // LANES, rows, LANES), jnp.float32),
        pltpu.VMEM((rows, channels), jnp.float32),
        pltpu.VMEM((rows, channels), jnp.float32),
        pltpu.VMEM((rows, channels), jnp.bfloat16),
        pltpu.VMEM((rows, channels), jnp.bfloat16),
        pltpu.VMEM((features // LANES, rows, LANES), jnp.float32),
        pltpu.SemaphoreType.DMA((2,)),
    ]
    params = pltpu.CompilerParams(vmem_limit_bytes=24 * 2**20)
    states, total, scale, shift, coefs = pl.pallas_call(
        functools.partial(first_kernel, width),
        out_shape=(
            shape(width, patches, features),
            shape(patches, features),
            shape(width, channels),
            shape(width, channels),
            shape(COEFS, width, LANES),
        ),
        in_specs=[anywhere, anywhere] + [vmem] * 7,
        out_specs=(vmem,) * 5,
        scratch_shapes=[pltpu.VMEM((patches, features), jnp.float32)] + work,
        compiler_params=params,
        name="first",
    )(
        start_state,
        noise,
        marks,
        jnp.asarray(noise_table()),
        input_weight,
        embed_weight,
        first_weight,
        second_weight,
        output_weight,
    )
    sums, total = pl.pallas_call(
        functools.partial(second_kernel, width),
        out_shape=(shape(width, patches, features), shape(patches, features)),
        in_specs=[vmem, vmem, anywhere] + [vmem] * 7,
        out_specs=(vmem,) * 2,
        scratch_shapes=work,
        compiler_params=params,
        name="second",
    )(
        states,
        earlier_blocks(total, count, width),
        noise,
        scale,
        shift,
        coefs,
        input_weight,
        first_weight,
        second_weight,
        output_weight,
    )
    return exchange(sums + earlier_blocks(total, count, width))[None]


def solution(mesh):
    return jax.shard_map(
        shards,
        mesh=mesh,
        in_specs=(
            P("groups", None, None),
            P(("groups", "steps", "inner"), None, None, None),
            P(("groups", "steps", "inner")),
            P("groups"),
            P(),
            P(),
            P(),
            P(),
            P(),
        ),
        out_specs=P(("groups", "steps", "inner"), None, None, None),
        check_vma=False,
    )
```

```python
import functools
import math

import jax
import jax.numpy as jnp
import numpy as np
from jax import lax
from jax.experimental import pallas as pl
from jax.experimental.pallas import tpu as pltpu
from jax.sharding import PartitionSpec as P

GROUPS = 32
TRAIN_STEPS = 1000
TIME = ("steps", "inner")
LANES = 128
CHUNK = 256
COEFS = 5
SPLIT = 2


def noise_table():
    levels = np.arange(TRAIN_STEPS, dtype=np.float64)
    betas = 0.0001 + (0.02 - 0.0001) * levels / (TRAIN_STEPS - 1)
    padded = np.zeros((1, -(-TRAIN_STEPS // LANES) * LANES), np.float32)
    padded[0, :TRAIN_STEPS] = np.exp(np.cumsum(np.log1p(-betas)))
    return padded


def group_mean(sums, size, count):
    lane = lax.broadcasted_iota(jnp.int32, sums.shape, 1)
    reach = 1
    while reach < size:
        upper = (lane & reach) != 0
        sums = sums + jnp.where(
            upper, pltpu.roll(sums, reach, 1), pltpu.roll(sums, LANES - reach, 1)
        )
        reach *= 2
    return sums * (1.0 / count)


def norm_silu(hidden_ref, act_ref, first, times, size, scale_ref, shift_ref):
    rows = hidden_ref.shape[0]
    patches = rows // times
    for lane in range(first, first + CHUNK, LANES):
        columns = slice(lane, lane + LANES)
        values = hidden_ref[:, columns].reshape(patches, times, LANES)
        mean = group_mean(jnp.sum(values, axis=0), size, patches * size)
        offset = values - mean
        spread = group_mean(jnp.sum(offset * offset, axis=0), size, patches * size)
        gain = 0.5 * lax.rsqrt(spread + 1e-05)
        if scale_ref is None:
            half = offset * gain
        else:
            gain = gain * (1.0 + scale_ref[:, columns])
            half = offset * gain + 0.5 * shift_ref[:, columns]
        act = half * jnp.tanh(half) + half
        act_ref[:, columns] = act.reshape(rows, LANES).astype(jnp.bfloat16)


def dot(left, right):
    return jnp.dot(left, right, preferred_element_type=jnp.float32)


def first_stage(times, rows_ref, scale_ref, shift_ref, input_weight, copies, next_copies, entry_ref, one_ref):
    features, channels = input_weight.shape
    flat = jnp.concatenate([rows_ref[block] for block in range(features // LANES)], axis=1)
    flat = flat.astype(jnp.bfloat16)
    wait_all(copies)
    for parts in next_copies:
        start_all(parts)
    for first in range(0, channels, CHUNK):
        columns = slice(first, first + CHUNK)
        entry_ref[:, columns] = dot(flat, input_weight[:, columns])
        norm_silu(entry_ref, one_ref, first, times, channels // GROUPS, scale_ref, shift_ref)


def later_stages(times, weights, copies, add_entry, hidden_ref, one_ref, two_ref, eps_ref):
    first_weight, second_weight, output_weight = weights
    channels, features = output_weight.shape
    size = channels // GROUPS
    wait_all(copies[0])
    for first in range(0, channels, CHUNK):
        columns = slice(first, first + CHUNK)
        hidden_ref[:, columns] = dot(one_ref[...], first_weight[:, columns])
        norm_silu(hidden_ref, two_ref, first, times, size, None, None)
    wait_all(copies[1])
    for first in range(0, channels, CHUNK):
        columns = slice(first, first + CHUNK)
        hidden_ref[:, columns] = add_entry(columns, dot(two_ref[...], second_weight[:, columns]))
        norm_silu(hidden_ref, one_ref, first, times, size, None, None)
    wait_all(copies[2])
    for first in range(0, features, CHUNK):
        part = dot(one_ref[...], output_weight[:, first : first + CHUNK])
        for lane in range(0, CHUNK, LANES):
            eps_ref[(first + lane) // LANES] = part[:, lane : lane + LANES]


def coefficients(now, later):
    ratio = (1.0 - later) / (1.0 - now)
    keep = ratio * jnp.sqrt(now / later)
    return (
        1.0 / jnp.sqrt(now),
        jnp.sqrt((1.0 - now) / now),
        (later - now) / (jnp.sqrt(later) * (1.0 - now)),
        keep - 1.0,
        jnp.sqrt(ratio * (1.0 - now / later)),
    )


def drift(state, eps, noise, coefs):
    inverse, slope, clean_part, state_part, sigma = coefs
    clean = jnp.clip(inverse * state - slope * eps, -1.0, 1.0)
    return clean_part * clean + state_part * state + sigma * noise


def plan_copies(sources, targets, sems):
    copies = []
    for index, (source, target) in enumerate(zip(sources, targets)):
        step = source.shape[0] // SPLIT
        parts = [
            pltpu.make_async_copy(
                source.at[pl.ds(part * step, step)],
                target.at[pl.ds(part * step, step)],
                sems.at[index * SPLIT + part],
            )
            for part in range(SPLIT)
        ]
        copies.append(parts)
    return copies


def start_all(parts):
    for part in parts:
        part.start()


def wait_all(parts):
    for part in parts:
        part.wait()


def spread_rows(rows_ref, step, stride, values):
    patches, features = values.shape
    for block in range(features // LANES):
        part = values[:, block * LANES : (block + 1) * LANES]
        rows_ref[block, pl.ds(step, patches, stride), :] = part


def prepare_kernel(
    width,
    start_hbm,
    input_hbm,
    gaps_ref,
    opening_ref,
    own_ref,
    entry_ref,
    norm_ref,
    part_ref,
    input_ref,
    own_sem,
    sems,
):
    place = lax.axis_index(TIME)
    own_copy = pltpu.make_async_copy(start_hbm.at[lax.rem(place, width)], own_ref, own_sem)
    own_copy.start()
    (copies,) = plan_copies((input_hbm,), (input_ref,), sems)
    start_all(copies)
    later = lax.broadcasted_iota(jnp.int32, part_ref.shape, 1) > place
    opening = jnp.where(place == 0, opening_ref[0], 0)
    part_ref[...] = opening - jnp.where(later, gaps_ref[0], 0)
    own_copy.wait()
    patches = own_ref.shape[0]
    channels = input_ref.shape[1]
    size = channels // GROUPS
    flat = own_ref[...].astype(jnp.bfloat16)
    wait_all(copies)
    for first in range(0, channels, CHUNK):
        columns = slice(first, first + CHUNK)
        entry_ref[:, columns] = dot(flat, input_ref[:, columns])
        for lane in range(first, first + CHUNK, LANES):
            columns = slice(lane, lane + LANES)
            values = entry_ref[:, columns]

            def mean(part):
                sums = jnp.sum(part, axis=0, keepdims=True)
                sums = jnp.broadcast_to(sums, (width, LANES))
                return group_mean(sums, size, patches * size)[:1]

            offset = values - mean(values)
            norm_ref[:, columns] = offset * lax.rsqrt(mean(offset * offset) + 1e-05)


def first_kernel(
    width,
    own_ref,
    entry_ref,
    norm_ref,
    noise_ref,
    marks_ref,
    table_ref,
    embed_hbm,
    first_hbm,
    second_hbm,
    output_hbm,
    state_ref,
    total_ref,
    scale_ref,
    shift_ref,
    coef_ref,
    hidden_ref,
    one_ref,
    two_ref,
    eps_ref,
    embed_ref,
    first_ref,
    second_ref,
    output_ref,
    sems,
):
    embed_copies, *copies = plan_copies(
        (embed_hbm, first_hbm, second_hbm, output_hbm),
        (embed_ref, first_ref, second_ref, output_ref),
        sems,
    )
    start_all(embed_copies)
    start_all(copies[0])
    place = lax.axis_index(TIME)
    image = lax.rem(place, width)
    patches, features = own_ref.shape
    lane = lax.broadcasted_iota(jnp.int32, (width, marks_ref.shape[1]), 1)
    time = lax.broadcasted_iota(jnp.int32, lane.shape, 0)
    marks = marks_ref[...].astype(jnp.float32)
    spot = place - image + time
    now_mark = jnp.sum(jnp.where(lane == spot, marks, 0.0), axis=1, keepdims=True)
    next_mark = jnp.sum(jnp.where(lane == spot + 1, marks, 0.0), axis=1, keepdims=True)
    level = lax.broadcasted_iota(jnp.int32, (width, table_ref.shape[1]), 1).astype(jnp.float32)
    table = table_ref[...]
    now = jnp.sum(jnp.where(level == now_mark, table, 0.0), axis=1, keepdims=True)
    later = jnp.sum(jnp.where(level == next_mark, table, 0.0), axis=1, keepdims=True)
    coefs = coefficients(now, later)
    for index, coef in enumerate(coefs):
        coef_ref[index] = jnp.broadcast_to(coef, (width, LANES))

    half = embed_ref.shape[0] // 2
    order = lax.broadcasted_iota(jnp.int32, (1, half), 1).astype(jnp.float32)
    angles = now_mark * jnp.exp(-math.log(10000.0) * order / half)
    channels = norm_ref.shape[1]
    cosine = jnp.cos(angles).astype(jnp.bfloat16)
    sine = jnp.sin(angles).astype(jnp.bfloat16)
    both = jnp.concatenate([cosine, sine], axis=1)
    wait_all(embed_copies)
    start_all(copies[1])
    start_all(copies[2])
    scale_ref[...] = dot(both, embed_ref[:, :channels])
    shift_ref[...] = dot(both, embed_ref[:, channels:])

    for lane in range(0, channels, LANES):
        columns = slice(lane, lane + LANES)
        gain = 0.5 * (1.0 + scale_ref[:, columns])
        lift = 0.5 * shift_ref[:, columns]
        half = norm_ref[:, columns][:, None, :] * gain[None] + lift[None]
        act = half * jnp.tanh(half) + half
        one_ref[:, columns] = act.reshape(patches * width, LANES).astype(jnp.bfloat16)

    def add_entry(columns, part):
        entry = entry_ref[:, columns]
        return (part.reshape(patches, width, -1) + entry[:, None, :]).reshape(part.shape)

    weights = (first_ref, second_ref, output_ref)
    later_stages(width, weights, copies, add_entry, hidden_ref, one_ref, two_ref, eps_ref)
    for block in range(features // LANES):
        columns = slice(block * LANES, (block + 1) * LANES)
        base = own_ref[:, columns]
        running = None
        for step in range(width):
            eps = eps_ref[block, pl.ds(step, patches, width), :]
            row = [coef_ref[index, step : step + 1, :] for index in range(COEFS)]
            state_ref[step, :, columns] = base if running is None else base + running
            change = drift(base, eps, noise_ref[step, :, columns], row)
            running = change if running is None else running + change
        total_ref[:, columns] = running


def second_kernel(
    width,
    state_ref,
    earlier_ref,
    noise_ref,
    scale_ref,
    shift_ref,
    coef_ref,
    input_ref,
    first_hbm,
    second_hbm,
    output_hbm,
    sum_ref,
    total_ref,
    rows_ref,
    entry_ref,
    hidden_ref,
    one_ref,
    two_ref,
    eps_ref,
    first_ref,
    second_ref,
    output_ref,
    sems,
):
    weights = (first_ref, second_ref, output_ref)
    copies = plan_copies((first_hbm, second_hbm, output_hbm), weights, sems)
    patches, features = earlier_ref.shape
    for step in range(width):
        spread_rows(rows_ref, step, width, state_ref[step] + earlier_ref[...])
    first_stage(
        width, rows_ref, scale_ref, shift_ref, input_ref, (), copies, entry_ref, one_ref
    )

    def add_entry(columns, part):
        return entry_ref[:, columns] + part

    later_stages(width, weights, copies, add_entry, hidden_ref, one_ref, two_ref, eps_ref)
    for block in range(features // LANES):
        columns = slice(block * LANES, (block + 1) * LANES)
        own = state_ref[0, :, columns]
        running = None
        for step in range(width):
            eps = eps_ref[block, pl.ds(step, patches, width), :]
            row = [coef_ref[index, step : step + 1, :] for index in range(COEFS)]
            state = state_ref[step, :, columns] + earlier_ref[:, columns]
            change = drift(state, eps, noise_ref[step, :, columns], row)
            running = change if running is None else running + change
            sum_ref[step, :, columns] = own + running
        total_ref[:, columns] = running


def shift_blocks(part, count, width, blocks):
    pairs = [(place, place + blocks * width) for place in range(count - blocks * width)]
    return lax.ppermute(part, TIME, pairs)


def earlier_blocks(part, count, width):
    total = shift_blocks(part, count, width, 1)
    reach = 1
    while reach < count // width - 1:
        total = total + shift_blocks(total, count, width, reach)
        reach *= 2
    return total


def shards(
    start_state,
    noise_draws,
    step_gaps,
    window_start,
    input_weight,
    embed_weight,
    first_weight,
    second_weight,
    output_weight,
):
    count = lax.axis_size(TIME)
    width, patches, features = start_state.shape
    channels = input_weight.shape[1]
    assert count % width == 0 and width % 8 == 0
    groups = [list(range(first, first + width)) for first in range(0, count, width)]
    def exchange(values):
        return lax.all_to_all(values, TIME, 0, 0, axis_index_groups=groups, tiled=True)

    noise = exchange(noise_draws[0])
    marks_length = -(-(count + 1) // LANES) * LANES

    def shape(*dims):
        return jax.ShapeDtypeStruct(dims, jnp.float32)

    vmem = pl.BlockSpec(memory_space=pltpu.VMEM)
    hbm = pl.BlockSpec(memory_space=pltpu.HBM)
    rows = width * patches
    blocked = pltpu.VMEM((features // LANES, rows, LANES), jnp.float32)
    wide = pltpu.VMEM((rows, channels), jnp.float32)
    act = pltpu.VMEM((rows, channels), jnp.bfloat16)

    def holder(weight):
        return pltpu.VMEM(weight.shape, weight.dtype)

    later = (first_weight, second_weight, output_weight)
    later_weights = [holder(weight) for weight in later]

    def limit(kib):
        return pltpu.CompilerParams(vmem_limit_bytes=kib * 1024)

    smem = pl.BlockSpec(memory_space=pltpu.SMEM)
    own, entry, norm, part = pl.pallas_call(
        functools.partial(prepare_kernel, width),
        out_shape=(
            shape(patches, features),
            shape(patches, channels),
            shape(patches, channels),
            jax.ShapeDtypeStruct((1, marks_length), jnp.int32),
        ),
        in_specs=[hbm] * 2 + [smem] * 2,
        out_specs=(vmem,) * 4,
        scratch_shapes=[
            holder(input_weight),
            pltpu.SemaphoreType.DMA,
            pltpu.SemaphoreType.DMA((SPLIT,)),
        ],
        compiler_params=limit(54800),
        name="prepare",
    )(start_state, input_weight, step_gaps, window_start)
    marks = lax.psum(part, TIME)
    states, total, scale, shift, coefs = pl.pallas_call(
        functools.partial(first_kernel, width),
        out_shape=(
            shape(width, patches, features),
            shape(patches, features),
            shape(width, channels),
            shape(width, channels),
            shape(COEFS, width, LANES),
        ),
        in_specs=[vmem] * 6 + [hbm] * 4,
        out_specs=(vmem,) * 5,
        scratch_shapes=[wide, act, act, blocked, holder(embed_weight), *later_weights]
        + [pltpu.SemaphoreType.DMA((4 * SPLIT,))],
        compiler_params=limit(52500),
        name="first",
    )(
        own,
        entry,
        norm,
        noise,
        marks,
        jnp.asarray(noise_table()),
        embed_weight,
        first_weight,
        second_weight,
        output_weight,
    )
    sums, total = pl.pallas_call(
        functools.partial(second_kernel, width),
        out_shape=(shape(width, patches, features), shape(patches, features)),
        in_specs=[vmem] * 7 + [hbm] * 3,
        out_specs=(vmem,) * 2,
        scratch_shapes=[blocked, wide, wide, act, act, blocked]
        + later_weights
        + [pltpu.SemaphoreType.DMA((4 * SPLIT,))],
        compiler_params=limit(50900),
        name="second",
    )(
        states,
        earlier_blocks(total, count, width),
        noise,
        scale,
        shift,
        coefs,
        input_weight,
        first_weight,
        second_weight,
        output_weight,
    )
    return exchange(sums + earlier_blocks(total, count, width))[None]


def solution(mesh):
    return jax.shard_map(
        shards,
        mesh=mesh,
        in_specs=(
            P("groups", None, None),
            P(("groups", "steps", "inner"), None, None, None),
            P(("groups", "steps", "inner")),
            P("groups"),
            P(),
            P(),
            P(),
            P(),
            P(),
        ),
        out_specs=P(("groups", "steps", "inner"), None, None, None),
        check_vma=False,
    )
```

```python
import functools
import math

import jax
import jax.numpy as jnp
import numpy as np
from jax import lax
from jax.experimental import pallas as pl
from jax.experimental.pallas import tpu as pltpu
from jax.sharding import PartitionSpec as P

GROUPS = 32
TRAIN_STEPS = 1000
TIME = ("steps", "inner")
LANES = 128
CHUNK = 256
COEFS = 5
SPLIT = 2


def noise_table():
    levels = np.arange(TRAIN_STEPS, dtype=np.float64)
    betas = 0.0001 + (0.02 - 0.0001) * levels / (TRAIN_STEPS - 1)
    padded = np.zeros((1, -(-TRAIN_STEPS // LANES) * LANES), np.float32)
    padded[0, :TRAIN_STEPS] = np.exp(np.cumsum(np.log1p(-betas)))
    return padded


def group_mean(sums, size, count):
    lane = lax.broadcasted_iota(jnp.int32, sums.shape, 1)
    reach = 1
    while reach < size:
        upper = (lane & reach) != 0
        sums = sums + jnp.where(
            upper, pltpu.roll(sums, reach, 1), pltpu.roll(sums, LANES - reach, 1)
        )
        reach *= 2
    return sums * (1.0 / count)


def norm_silu(hidden_ref, act_ref, first, times, size, scale_ref, shift_ref):
    rows = hidden_ref.shape[0]
    patches = rows // times
    for lane in range(first, first + CHUNK, LANES):
        columns = slice(lane, lane + LANES)
        values = hidden_ref[:, columns].reshape(patches, times, LANES)
        mean = group_mean(jnp.sum(values, axis=0), size, patches * size)
        offset = values - mean
        spread = group_mean(jnp.sum(offset * offset, axis=0), size, patches * size)
        gain = 0.5 * lax.rsqrt(spread + 1e-05)
        if scale_ref is None:
            half = offset * gain
        else:
            gain = gain * (1.0 + scale_ref[:, columns])
            half = offset * gain + 0.5 * shift_ref[:, columns]
        act = half * jnp.tanh(half) + half
        act_ref[:, columns] = act.reshape(rows, LANES).astype(jnp.bfloat16)


def dot(left, right):
    return jnp.dot(left, right, preferred_element_type=jnp.float32)


def first_stage(times, rows_ref, scale_ref, shift_ref, input_weight, copies, next_copies, entry_ref, one_ref):
    features, channels = input_weight.shape
    flat = jnp.concatenate([rows_ref[block] for block in range(features // LANES)], axis=1)
    flat = flat.astype(jnp.bfloat16)
    wait_all(copies)
    for parts in next_copies:
        start_all(parts)
    for first in range(0, channels, CHUNK):
        columns = slice(first, first + CHUNK)
        entry_ref[:, columns] = dot(flat, input_weight[:, columns])
        norm_silu(entry_ref, one_ref, first, times, channels // GROUPS, scale_ref, shift_ref)


def later_stages(times, weights, copies, add_entry, hidden_ref, one_ref, two_ref, eps_ref):
    first_weight, second_weight, output_weight = weights
    channels, features = output_weight.shape
    size = channels // GROUPS
    wait_all(copies[0])
    for first in range(0, channels, CHUNK):
        columns = slice(first, first + CHUNK)
        hidden_ref[:, columns] = dot(one_ref[...], first_weight[:, columns])
        norm_silu(hidden_ref, two_ref, first, times, size, None, None)
    wait_all(copies[1])
    for first in range(0, channels, CHUNK):
        columns = slice(first, first + CHUNK)
        hidden_ref[:, columns] = add_entry(columns, dot(two_ref[...], second_weight[:, columns]))
        norm_silu(hidden_ref, one_ref, first, times, size, None, None)
    wait_all(copies[2])
    for first in range(0, features, CHUNK):
        part = dot(one_ref[...], output_weight[:, first : first + CHUNK])
        for lane in range(0, CHUNK, LANES):
            eps_ref[(first + lane) // LANES] = part[:, lane : lane + LANES]


def coefficients(now, later):
    ratio = (1.0 - later) / (1.0 - now)
    keep = ratio * jnp.sqrt(now / later)
    return (
        1.0 / jnp.sqrt(now),
        jnp.sqrt((1.0 - now) / now),
        (later - now) / (jnp.sqrt(later) * (1.0 - now)),
        keep - 1.0,
        jnp.sqrt(ratio * (1.0 - now / later)),
    )


def drift(state, eps, noise, coefs):
    inverse, slope, clean_part, state_part, sigma = coefs
    clean = jnp.clip(inverse * state - slope * eps, -1.0, 1.0)
    return clean_part * clean + state_part * state + sigma * noise


def plan_copies(sources, targets, sems):
    copies = []
    for index, (source, target) in enumerate(zip(sources, targets)):
        step = source.shape[0] // SPLIT
        parts = [
            pltpu.make_async_copy(
                source.at[pl.ds(part * step, step)],
                target.at[pl.ds(part * step, step)],
                sems.at[index * SPLIT + part],
            )
            for part in range(SPLIT)
        ]
        copies.append(parts)
    return copies


def start_all(parts):
    for part in parts:
        part.start()


def wait_all(parts):
    for part in parts:
        part.wait()


def spread_rows(rows_ref, step, stride, values):
    patches, features = values.shape
    for block in range(features // LANES):
        part = values[:, block * LANES : (block + 1) * LANES]
        rows_ref[block, pl.ds(step, patches, stride), :] = part


def prepare_kernel(
    width,
    start_hbm,
    input_hbm,
    gaps_ref,
    opening_ref,
    own_ref,
    entry_ref,
    norm_ref,
    part_ref,
    input_ref,
    own_sem,
    sems,
):
    place = lax.axis_index(TIME)
    own_copy = pltpu.make_async_copy(start_hbm.at[lax.rem(place, width)], own_ref, own_sem)
    own_copy.start()
    (copies,) = plan_copies((input_hbm,), (input_ref,), sems)
    start_all(copies)
    later = lax.broadcasted_iota(jnp.int32, part_ref.shape, 1) > place
    opening = jnp.where(place == 0, opening_ref[0], 0)
    part_ref[...] = opening - jnp.where(later, gaps_ref[0], 0)
    own_copy.wait()
    patches = own_ref.shape[0]
    channels = input_ref.shape[1]
    size = channels // GROUPS
    flat = own_ref[...].astype(jnp.bfloat16)
    wait_all(copies)
    for first in range(0, channels, CHUNK):
        columns = slice(first, first + CHUNK)
        entry_ref[:, columns] = dot(flat, input_ref[:, columns])
        for lane in range(first, first + CHUNK, LANES):
            columns = slice(lane, lane + LANES)
            values = entry_ref[:, columns]

            def mean(part):
                sums = jnp.sum(part, axis=0, keepdims=True)
                sums = jnp.broadcast_to(sums, (width, LANES))
                return group_mean(sums, size, patches * size)[:1]

            offset = values - mean(values)
            norm_ref[:, columns] = offset * lax.rsqrt(mean(offset * offset) + 1e-05)


def first_kernel(
    width,
    own_ref,
    entry_ref,
    norm_ref,
    noise_ref,
    marks_ref,
    table_ref,
    embed_hbm,
    first_hbm,
    second_hbm,
    output_hbm,
    state_ref,
    total_ref,
    scale_ref,
    shift_ref,
    coef_ref,
    hidden_ref,
    one_ref,
    two_ref,
    eps_ref,
    embed_ref,
    first_ref,
    second_ref,
    output_ref,
    sems,
):
    embed_copies, *copies = plan_copies(
        (embed_hbm, first_hbm, second_hbm, output_hbm),
        (embed_ref, first_ref, second_ref, output_ref),
        sems,
    )
    start_all(embed_copies)
    start_all(copies[0])
    place = lax.axis_index(TIME)
    image = lax.rem(place, width)
    patches, features = own_ref.shape
    lane = lax.broadcasted_iota(jnp.int32, (width, marks_ref.shape[1]), 1)
    time = lax.broadcasted_iota(jnp.int32, lane.shape, 0)
    marks = marks_ref[...].astype(jnp.float32)
    spot = place - image + time
    now_mark = jnp.sum(jnp.where(lane == spot, marks, 0.0), axis=1, keepdims=True)
    next_mark = jnp.sum(jnp.where(lane == spot + 1, marks, 0.0), axis=1, keepdims=True)
    level = lax.broadcasted_iota(jnp.int32, (width, table_ref.shape[1]), 1).astype(jnp.float32)
    table = table_ref[...]
    now = jnp.sum(jnp.where(level == now_mark, table, 0.0), axis=1, keepdims=True)
    later = jnp.sum(jnp.where(level == next_mark, table, 0.0), axis=1, keepdims=True)
    coefs = coefficients(now, later)
    for index, coef in enumerate(coefs):
        coef_ref[index] = jnp.broadcast_to(coef, (width, LANES))

    half = embed_ref.shape[0] // 2
    order = lax.broadcasted_iota(jnp.int32, (1, half), 1).astype(jnp.float32)
    angles = now_mark * jnp.exp(-math.log(10000.0) * order / half)
    channels = norm_ref.shape[1]
    cosine = jnp.cos(angles).astype(jnp.bfloat16)
    sine = jnp.sin(angles).astype(jnp.bfloat16)
    both = jnp.concatenate([cosine, sine], axis=1)
    wait_all(embed_copies)
    start_all(copies[1])
    start_all(copies[2])
    scale_ref[...] = dot(both, embed_ref[:, :channels])
    shift_ref[...] = dot(both, embed_ref[:, channels:])

    for lane in range(0, channels, LANES):
        columns = slice(lane, lane + LANES)
        gain = 0.5 * (1.0 + scale_ref[:, columns])
        lift = 0.5 * shift_ref[:, columns]
        half = norm_ref[:, columns][:, None, :] * gain[None] + lift[None]
        act = half * jnp.tanh(half) + half
        one_ref[:, columns] = act.reshape(patches * width, LANES).astype(jnp.bfloat16)

    def add_entry(columns, part):
        entry = entry_ref[:, columns]
        return (part.reshape(patches, width, -1) + entry[:, None, :]).reshape(part.shape)

    weights = (first_ref, second_ref, output_ref)
    later_stages(width, weights, copies, add_entry, hidden_ref, one_ref, two_ref, eps_ref)
    for block in range(features // LANES):
        columns = slice(block * LANES, (block + 1) * LANES)
        base = own_ref[:, columns]
        running = None
        for step in range(width):
            eps = eps_ref[block, pl.ds(step, patches, width), :]
            row = [coef_ref[index, step : step + 1, :] for index in range(COEFS)]
            state_ref[step, :, columns] = base if running is None else base + running
            change = drift(base, eps, noise_ref[step, :, columns], row)
            running = change if running is None else running + change
        total_ref[:, columns] = running


def early_kernel(width, *refs):
    @pl.when(lax.axis_index(TIME) < width)
    def _():
        second_kernel(width, refs[0], None, *refs[1:])


def late_kernel(width, sums_ref, *refs):
    @pl.when(lax.axis_index(TIME) >= width)
    def _():
        second_kernel(width, *refs[:11], None, *refs[11:])


def second_kernel(
    width,
    state_ref,
    earlier_ref,
    noise_ref,
    scale_ref,
    shift_ref,
    coef_ref,
    input_ref,
    first_hbm,
    second_hbm,
    output_hbm,
    sum_ref,
    total_ref,
    rows_ref,
    entry_ref,
    hidden_ref,
    one_ref,
    two_ref,
    eps_ref,
    first_ref,
    second_ref,
    output_ref,
    sems,
):
    weights = (first_ref, second_ref, output_ref)
    copies = plan_copies((first_hbm, second_hbm, output_hbm), weights, sems)
    _, patches, features = state_ref.shape

    def state_of(step, columns):
        state = state_ref[step, :, columns]
        return state if earlier_ref is None else state + earlier_ref[:, columns]

    for step in range(width):
        spread_rows(rows_ref, step, width, state_of(step, slice(None)))
    first_stage(
        width, rows_ref, scale_ref, shift_ref, input_ref, (), copies, entry_ref, one_ref
    )

    def add_entry(columns, part):
        return entry_ref[:, columns] + part

    later_stages(width, weights, copies, add_entry, hidden_ref, one_ref, two_ref, eps_ref)
    for block in range(features // LANES):
        columns = slice(block * LANES, (block + 1) * LANES)
        own = state_ref[0, :, columns]
        running = None
        for step in range(width):
            eps = eps_ref[block, pl.ds(step, patches, width), :]
            row = [coef_ref[index, step : step + 1, :] for index in range(COEFS)]
            change = drift(state_of(step, columns), eps, noise_ref[step, :, columns], row)
            running = change if running is None else running + change
            sum_ref[step, :, columns] = own + running
        if total_ref is not None:
            total_ref[:, columns] = running


def shift_blocks(part, count, width, blocks):
    pairs = [(place, place + blocks * width) for place in range(count - blocks * width)]
    return lax.ppermute(part, TIME, pairs)


def earlier_blocks(part, count, width):
    total = shift_blocks(part, count, width, 1)
    reach = 1
    while reach < count // width - 1:
        total = total + shift_blocks(total, count, width, reach)
        reach *= 2
    return total


def shards(
    start_state,
    noise_draws,
    step_gaps,
    window_start,
    input_weight,
    embed_weight,
    first_weight,
    second_weight,
    output_weight,
):
    count = lax.axis_size(TIME)
    width, patches, features = start_state.shape
    channels = input_weight.shape[1]
    assert count % width == 0 and width % 8 == 0
    groups = [list(range(first, first + width)) for first in range(0, count, width)]
    def exchange(values):
        return lax.all_to_all(values, TIME, 0, 0, axis_index_groups=groups, tiled=True)

    noise = exchange(noise_draws[0])
    marks_length = -(-(count + 1) // LANES) * LANES

    def shape(*dims):
        return jax.ShapeDtypeStruct(dims, jnp.float32)

    vmem = pl.BlockSpec(memory_space=pltpu.VMEM)
    hbm = pl.BlockSpec(memory_space=pltpu.HBM)
    rows = width * patches
    blocked = pltpu.VMEM((features // LANES, rows, LANES), jnp.float32)
    wide = pltpu.VMEM((rows, channels), jnp.float32)
    act = pltpu.VMEM((rows, channels), jnp.bfloat16)

    def holder(weight):
        return pltpu.VMEM(weight.shape, weight.dtype)

    later = (first_weight, second_weight, output_weight)
    later_weights = [holder(weight) for weight in later]

    def limit(kib):
        return pltpu.CompilerParams(vmem_limit_bytes=kib * 1024)

    smem = pl.BlockSpec(memory_space=pltpu.SMEM)
    own, entry, norm, part = pl.pallas_call(
        functools.partial(prepare_kernel, width),
        out_shape=(
            shape(patches, features),
            shape(patches, channels),
            shape(patches, channels),
            jax.ShapeDtypeStruct((1, marks_length), jnp.int32),
        ),
        in_specs=[hbm] * 2 + [smem] * 2,
        out_specs=(vmem,) * 4,
        scratch_shapes=[
            holder(input_weight),
            pltpu.SemaphoreType.DMA,
            pltpu.SemaphoreType.DMA((SPLIT,)),
        ],
        compiler_params=limit(54800),
        name="prepare",
    )(start_state, input_weight, step_gaps, window_start)
    marks = lax.psum(part, TIME)
    states, total, scale, shift, coefs = pl.pallas_call(
        functools.partial(first_kernel, width),
        out_shape=(
            shape(width, patches, features),
            shape(patches, features),
            shape(width, channels),
            shape(width, channels),
            shape(COEFS, width, LANES),
        ),
        in_specs=[vmem] * 6 + [hbm] * 4,
        out_specs=(vmem,) * 5,
        scratch_shapes=[wide, act, act, blocked, holder(embed_weight), *later_weights]
        + [pltpu.SemaphoreType.DMA((4 * SPLIT,))],
        compiler_params=limit(52500),
        name="first",
    )(
        own,
        entry,
        norm,
        noise,
        marks,
        jnp.asarray(noise_table()),
        embed_weight,
        first_weight,
        second_weight,
        output_weight,
    )
    scratch = [blocked, wide, wide, act, act, blocked, *later_weights]
    scratch.append(pltpu.SemaphoreType.DMA((4 * SPLIT,)))
    sums_shape = shape(width, patches, features)
    total_shape = shape(patches, features)
    common = (noise, scale, shift, coefs, input_weight, *later)
    flops = 2 * rows * channels * (2 * features + 2 * channels)
    cost = pl.CostEstimate(flops=flops, transcendentals=0, bytes_accessed=8 * 2**20)
    if count != 2 * width:
        sums, total = pl.pallas_call(
            functools.partial(second_kernel, width),
            out_shape=(sums_shape, total_shape),
            in_specs=[vmem] * 7 + [hbm] * 3,
            out_specs=(vmem,) * 2,
            scratch_shapes=scratch,
            compiler_params=limit(50900),
            name="second",
        )(states, earlier_blocks(total, count, width), *common)
        return exchange(sums + earlier_blocks(total, count, width))[None]
    earlier = earlier_blocks(total, count, width)
    sums, total = pl.pallas_call(
        functools.partial(early_kernel, width),
        out_shape=(sums_shape, total_shape),
        in_specs=[vmem] * 6 + [hbm] * 3,
        out_specs=(vmem,) * 2,
        scratch_shapes=scratch,
        cost_estimate=cost,
        compiler_params=limit(50900),
        name="early",
    )(states, *common)
    moved = earlier_blocks(total, count, width)
    sums = pl.pallas_call(
        functools.partial(late_kernel, width),
        out_shape=sums_shape,
        in_specs=[vmem] * 8 + [hbm] * 3,
        out_specs=vmem,
        scratch_shapes=scratch,
        input_output_aliases={0: 0},
        cost_estimate=cost,
        compiler_params=limit(50900),
        name="late",
    )(sums, states, earlier, *common)
    return exchange(sums + moved)[None]


def solution(mesh):
    return jax.shard_map(
        shards,
        mesh=mesh,
        in_specs=(
            P("groups", None, None),
            P(("groups", "steps", "inner"), None, None, None),
            P(("groups", "steps", "inner")),
            P("groups"),
            P(),
            P(),
            P(),
            P(),
            P(),
        ),
        out_specs=P(("groups", "steps", "inner"), None, None, None),
        check_vma=False,
    )
```

```python
import functools
import math

import jax
import jax.numpy as jnp
import numpy as np
from jax import lax
from jax.experimental import pallas as pl
from jax.experimental.pallas import tpu as pltpu
from jax.sharding import PartitionSpec as P

GROUPS = 32
TRAIN_STEPS = 1000
TIME = ("steps", "inner")
LANES = 128
CHUNK = 256
COEFS = 5
SPLIT = 1


def noise_table():
    levels = np.arange(TRAIN_STEPS, dtype=np.float64)
    betas = 0.0001 + (0.02 - 0.0001) * levels / (TRAIN_STEPS - 1)
    padded = np.zeros((1, -(-TRAIN_STEPS // LANES) * LANES), np.float32)
    padded[0, :TRAIN_STEPS] = np.exp(np.cumsum(np.log1p(-betas)))
    return padded


def group_mean(sums, size, count):
    lane = lax.broadcasted_iota(jnp.int32, sums.shape, 1)
    reach = 1
    while reach < size:
        upper = (lane & reach) != 0
        sums = sums + jnp.where(
            upper, pltpu.roll(sums, reach, 1), pltpu.roll(sums, LANES - reach, 1)
        )
        reach *= 2
    return sums * (1.0 / count)


def norm_silu(hidden_ref, act_ref, first, times, size, scale_ref, shift_ref):
    rows = hidden_ref.shape[0]
    patches = rows // times
    for lane in range(first, first + CHUNK, LANES):
        columns = slice(lane, lane + LANES)
        values = hidden_ref[:, columns].reshape(patches, times, LANES)
        mean = group_mean(jnp.sum(values, axis=0), size, patches * size)
        offset = values - mean
        spread = group_mean(jnp.sum(offset * offset, axis=0), size, patches * size)
        gain = 0.5 * lax.rsqrt(spread + 1e-05)
        if scale_ref is None:
            half = offset * gain
        else:
            gain = gain * (1.0 + scale_ref[:, columns])
            half = offset * gain + 0.5 * shift_ref[:, columns]
        act = half * jnp.tanh(half) + half
        act_ref[:, columns] = act.reshape(rows, LANES).astype(jnp.bfloat16)


def dot(left, right):
    return jnp.dot(left, right, preferred_element_type=jnp.float32)


def first_stage(times, rows_ref, scale_ref, shift_ref, input_weight, copies, next_copies, entry_ref, one_ref):
    features, channels = input_weight.shape
    flat = jnp.concatenate([rows_ref[block] for block in range(features // LANES)], axis=1)
    flat = flat.astype(jnp.bfloat16)
    wait_all(copies)
    for parts in next_copies:
        start_all(parts)
    for first in range(0, channels, CHUNK):
        columns = slice(first, first + CHUNK)
        entry_ref[:, columns] = dot(flat, input_weight[:, columns])
        norm_silu(entry_ref, one_ref, first, times, channels // GROUPS, scale_ref, shift_ref)


def later_stages(times, weights, copies, add_entry, hidden_ref, one_ref, two_ref, eps_ref):
    first_weight, second_weight, output_weight = weights
    channels, features = output_weight.shape
    size = channels // GROUPS
    wait_all(copies[0])
    for first in range(0, channels, CHUNK):
        columns = slice(first, first + CHUNK)
        hidden_ref[:, columns] = dot(one_ref[...], first_weight[:, columns])
        norm_silu(hidden_ref, two_ref, first, times, size, None, None)
    wait_all(copies[1])
    for first in range(0, channels, CHUNK):
        columns = slice(first, first + CHUNK)
        hidden_ref[:, columns] = add_entry(columns, dot(two_ref[...], second_weight[:, columns]))
        norm_silu(hidden_ref, one_ref, first, times, size, None, None)
    wait_all(copies[2])
    for first in range(0, features, CHUNK):
        part = dot(one_ref[...], output_weight[:, first : first + CHUNK])
        for lane in range(0, CHUNK, LANES):
            eps_ref[(first + lane) // LANES] = part[:, lane : lane + LANES]


def coefficients(now, later):
    ratio = (1.0 - later) / (1.0 - now)
    keep = ratio * jnp.sqrt(now / later)
    return (
        1.0 / jnp.sqrt(now),
        jnp.sqrt((1.0 - now) / now),
        (later - now) / (jnp.sqrt(later) * (1.0 - now)),
        keep - 1.0,
        jnp.sqrt(ratio * (1.0 - now / later)),
    )


def drift(state, eps, noise, coefs):
    inverse, slope, clean_part, state_part, sigma = coefs
    clean = jnp.clip(inverse * state - slope * eps, -1.0, 1.0)
    return clean_part * clean + state_part * state + sigma * noise


def plan_copies(sources, targets, sems):
    copies = []
    for index, (source, target) in enumerate(zip(sources, targets)):
        step = source.shape[0] // SPLIT
        parts = [
            pltpu.make_async_copy(
                source.at[pl.ds(part * step, step)],
                target.at[pl.ds(part * step, step)],
                sems.at[index * SPLIT + part],
            )
            for part in range(SPLIT)
        ]
        copies.append(parts)
    return copies


def start_all(parts):
    for part in parts:
        part.start()


def wait_all(parts):
    for part in parts:
        part.wait()


def spread_rows(rows_ref, step, stride, values):
    patches, features = values.shape
    for block in range(features // LANES):
        part = values[:, block * LANES : (block + 1) * LANES]
        rows_ref[block, pl.ds(step, patches, stride), :] = part


def prepare_kernel(
    width,
    start_hbm,
    input_hbm,
    gaps_ref,
    opening_ref,
    own_ref,
    entry_ref,
    norm_ref,
    part_ref,
    input_ref,
    own_sem,
    sems,
):
    place = lax.axis_index(TIME)
    own_copy = pltpu.make_async_copy(start_hbm.at[lax.rem(place, width)], own_ref, own_sem)
    own_copy.start()
    (copies,) = plan_copies((input_hbm,), (input_ref,), sems)
    start_all(copies)
    later = lax.broadcasted_iota(jnp.int32, part_ref.shape, 1) > place
    opening = jnp.where(place == 0, opening_ref[0], 0)
    part_ref[...] = opening - jnp.where(later, gaps_ref[0], 0)
    own_copy.wait()
    patches = own_ref.shape[0]
    channels = input_ref.shape[1]
    size = channels // GROUPS
    flat = own_ref[...].astype(jnp.bfloat16)
    wait_all(copies)
    for first in range(0, channels, CHUNK):
        columns = slice(first, first + CHUNK)
        entry_ref[:, columns] = dot(flat, input_ref[:, columns])
        for lane in range(first, first + CHUNK, LANES):
            columns = slice(lane, lane + LANES)
            values = entry_ref[:, columns]

            def mean(part):
                sums = jnp.sum(part, axis=0, keepdims=True)
                sums = jnp.broadcast_to(sums, (width, LANES))
                return group_mean(sums, size, patches * size)[:1]

            offset = values - mean(values)
            norm_ref[:, columns] = offset * lax.rsqrt(mean(offset * offset) + 1e-05)


def first_kernel(
    width,
    own_ref,
    entry_ref,
    norm_ref,
    noise_ref,
    marks_ref,
    table_ref,
    embed_hbm,
    first_hbm,
    second_hbm,
    output_hbm,
    state_ref,
    total_ref,
    scale_ref,
    shift_ref,
    coef_ref,
    hidden_ref,
    one_ref,
    two_ref,
    eps_ref,
    embed_ref,
    first_ref,
    second_ref,
    output_ref,
    sems,
):
    embed_copies, *copies = plan_copies(
        (embed_hbm, first_hbm, second_hbm, output_hbm),
        (embed_ref, first_ref, second_ref, output_ref),
        sems,
    )
    start_all(embed_copies)
    start_all(copies[0])
    place = lax.axis_index(TIME)
    image = lax.rem(place, width)
    patches, features = own_ref.shape
    lane = lax.broadcasted_iota(jnp.int32, (width, marks_ref.shape[1]), 1)
    time = lax.broadcasted_iota(jnp.int32, lane.shape, 0)
    marks = marks_ref[...].astype(jnp.float32)
    spot = place - image + time
    now_mark = jnp.sum(jnp.where(lane == spot, marks, 0.0), axis=1, keepdims=True)
    next_mark = jnp.sum(jnp.where(lane == spot + 1, marks, 0.0), axis=1, keepdims=True)
    level = lax.broadcasted_iota(jnp.int32, (width, table_ref.shape[1]), 1).astype(jnp.float32)
    table = table_ref[...]
    now = jnp.sum(jnp.where(level == now_mark, table, 0.0), axis=1, keepdims=True)
    later = jnp.sum(jnp.where(level == next_mark, table, 0.0), axis=1, keepdims=True)
    coefs = coefficients(now, later)
    for index, coef in enumerate(coefs):
        coef_ref[index] = jnp.broadcast_to(coef, (width, LANES))

    half = embed_ref.shape[0] // 2
    order = lax.broadcasted_iota(jnp.int32, (1, half), 1).astype(jnp.float32)
    angles = now_mark * jnp.exp(-math.log(10000.0) * order / half)
    channels = norm_ref.shape[1]
    cosine = jnp.cos(angles).astype(jnp.bfloat16)
    sine = jnp.sin(angles).astype(jnp.bfloat16)
    both = jnp.concatenate([cosine, sine], axis=1)
    wait_all(embed_copies)
    start_all(copies[1])
    start_all(copies[2])
    scale_ref[...] = dot(both, embed_ref[:, :channels])
    shift_ref[...] = dot(both, embed_ref[:, channels:])

    for lane in range(0, channels, LANES):
        columns = slice(lane, lane + LANES)
        gain = 0.5 * (1.0 + scale_ref[:, columns])
        lift = 0.5 * shift_ref[:, columns]
        half = norm_ref[:, columns][:, None, :] * gain[None] + lift[None]
        act = half * jnp.tanh(half) + half
        one_ref[:, columns] = act.reshape(patches * width, LANES).astype(jnp.bfloat16)

    def add_entry(columns, part):
        entry = entry_ref[:, columns]
        return (part.reshape(patches, width, -1) + entry[:, None, :]).reshape(part.shape)

    weights = (first_ref, second_ref, output_ref)
    later_stages(width, weights, copies, add_entry, hidden_ref, one_ref, two_ref, eps_ref)
    for block in range(features // LANES):
        columns = slice(block * LANES, (block + 1) * LANES)
        base = own_ref[:, columns]
        running = None
        for step in range(width):
            eps = eps_ref[block, pl.ds(step, patches, width), :]
            row = [coef_ref[index, step : step + 1, :] for index in range(COEFS)]
            state_ref[step, :, columns] = base if running is None else base + running
            change = drift(base, eps, noise_ref[step, :, columns], row)
            running = change if running is None else running + change
        total_ref[:, columns] = running


def early_kernel(width, *refs):
    @pl.when(lax.axis_index(TIME) < width)
    def _():
        second_kernel(width, refs[0], None, *refs[1:])


def late_kernel(width, sums_ref, *refs):
    @pl.when(lax.axis_index(TIME) >= width)
    def _():
        second_kernel(width, *refs[:11], None, *refs[11:])


def second_kernel(
    width,
    state_ref,
    earlier_ref,
    noise_ref,
    scale_ref,
    shift_ref,
    coef_ref,
    input_ref,
    first_hbm,
    second_hbm,
    output_hbm,
    sum_ref,
    total_ref,
    rows_ref,
    entry_ref,
    hidden_ref,
    one_ref,
    two_ref,
    eps_ref,
    first_ref,
    second_ref,
    output_ref,
    sems,
):
    weights = (first_ref, second_ref, output_ref)
    copies = plan_copies((first_hbm, second_hbm, output_hbm), weights, sems)
    _, patches, features = state_ref.shape

    def state_of(step, columns):
        state = state_ref[step, :, columns]
        return state if earlier_ref is None else state + earlier_ref[:, columns]

    for step in range(width):
        spread_rows(rows_ref, step, width, state_of(step, slice(None)))
    first_stage(
        width, rows_ref, scale_ref, shift_ref, input_ref, (), copies, entry_ref, one_ref
    )

    def add_entry(columns, part):
        return entry_ref[:, columns] + part

    later_stages(width, weights, copies, add_entry, hidden_ref, one_ref, two_ref, eps_ref)
    for block in range(features // LANES):
        columns = slice(block * LANES, (block + 1) * LANES)
        own = state_ref[0, :, columns]
        running = None
        for step in range(width):
            eps = eps_ref[block, pl.ds(step, patches, width), :]
            row = [coef_ref[index, step : step + 1, :] for index in range(COEFS)]
            change = drift(state_of(step, columns), eps, noise_ref[step, :, columns], row)
            running = change if running is None else running + change
            sum_ref[step, :, columns] = own + running
        if total_ref is not None:
            total_ref[:, columns] = running


def shift_blocks(part, count, width, blocks):
    pairs = [(place, place + blocks * width) for place in range(count - blocks * width)]
    return lax.ppermute(part, TIME, pairs)


def earlier_blocks(part, count, width):
    total = shift_blocks(part, count, width, 1)
    reach = 1
    while reach < count // width - 1:
        total = total + shift_blocks(total, count, width, reach)
        reach *= 2
    return total


def shards(
    start_state,
    noise_draws,
    step_gaps,
    window_start,
    input_weight,
    embed_weight,
    first_weight,
    second_weight,
    output_weight,
):
    count = lax.axis_size(TIME)
    width, patches, features = start_state.shape
    channels = input_weight.shape[1]
    assert count % width == 0 and width % 8 == 0
    groups = [list(range(first, first + width)) for first in range(0, count, width)]
    def exchange(values):
        return lax.all_to_all(values, TIME, 0, 0, axis_index_groups=groups, tiled=True)

    noise = exchange(noise_draws[0])
    marks_length = -(-(count + 1) // LANES) * LANES

    def shape(*dims):
        return jax.ShapeDtypeStruct(dims, jnp.float32)

    vmem = pl.BlockSpec(memory_space=pltpu.VMEM)
    hbm = pl.BlockSpec(memory_space=pltpu.HBM)
    rows = width * patches
    blocked = pltpu.VMEM((features // LANES, rows, LANES), jnp.float32)
    wide = pltpu.VMEM((rows, channels), jnp.float32)
    act = pltpu.VMEM((rows, channels), jnp.bfloat16)

    def holder(weight):
        return pltpu.VMEM(weight.shape, weight.dtype)

    later = (first_weight, second_weight, output_weight)
    later_weights = [holder(weight) for weight in later]

    def limit(kib):
        return pltpu.CompilerParams(vmem_limit_bytes=kib * 1024)

    smem = pl.BlockSpec(memory_space=pltpu.SMEM)
    own, entry, norm, part = pl.pallas_call(
        functools.partial(prepare_kernel, width),
        out_shape=(
            shape(patches, features),
            shape(patches, channels),
            shape(patches, channels),
            jax.ShapeDtypeStruct((1, marks_length), jnp.int32),
        ),
        in_specs=[hbm] * 2 + [smem] * 2,
        out_specs=(vmem,) * 4,
        scratch_shapes=[
            holder(input_weight),
            pltpu.SemaphoreType.DMA,
            pltpu.SemaphoreType.DMA((SPLIT,)),
        ],
        compiler_params=limit(54800),
        name="prepare",
    )(start_state, input_weight, step_gaps, window_start)
    marks = lax.psum(part, TIME)
    states, total, scale, shift, coefs = pl.pallas_call(
        functools.partial(first_kernel, width),
        out_shape=(
            shape(width, patches, features),
            shape(patches, features),
            shape(width, channels),
            shape(width, channels),
            shape(COEFS, width, LANES),
        ),
        in_specs=[vmem] * 6 + [hbm] * 4,
        out_specs=(vmem,) * 5,
        scratch_shapes=[wide, act, act, blocked, holder(embed_weight), *later_weights]
        + [pltpu.SemaphoreType.DMA((4 * SPLIT,))],
        compiler_params=limit(51300),
        name="first",
    )(
        own,
        entry,
        norm,
        noise,
        marks,
        jnp.asarray(noise_table()),
        embed_weight,
        first_weight,
        second_weight,
        output_weight,
    )
    scratch = [blocked, wide, wide, act, act, blocked, *later_weights]
    scratch.append(pltpu.SemaphoreType.DMA((4 * SPLIT,)))
    sums_shape = shape(width, patches, features)
    total_shape = shape(patches, features)
    common = (noise, scale, shift, coefs, input_weight, *later)
    flops = 2 * rows * channels * (2 * features + 2 * channels)
    cost = pl.CostEstimate(flops=flops, transcendentals=0, bytes_accessed=8 * 2**20)
    if count != 2 * width:
        sums, total = pl.pallas_call(
            functools.partial(second_kernel, width),
            out_shape=(sums_shape, total_shape),
            in_specs=[vmem] * 7 + [hbm] * 3,
            out_specs=(vmem,) * 2,
            scratch_shapes=scratch,
            compiler_params=limit(50900),
            name="second",
        )(states, earlier_blocks(total, count, width), *common)
        return exchange(sums + earlier_blocks(total, count, width))[None]
    earlier = earlier_blocks(total, count, width)
    sums, total = pl.pallas_call(
        functools.partial(early_kernel, width),
        out_shape=(sums_shape, total_shape),
        in_specs=[vmem] * 6 + [hbm] * 3,
        out_specs=(vmem,) * 2,
        scratch_shapes=scratch,
        cost_estimate=cost,
        compiler_params=limit(50900),
        name="early",
    )(states, *common)
    moved = earlier_blocks(total, count, width)
    sums = pl.pallas_call(
        functools.partial(late_kernel, width),
        out_shape=sums_shape,
        in_specs=[vmem] * 8 + [hbm] * 3,
        out_specs=vmem,
        scratch_shapes=scratch,
        input_output_aliases={0: 0},
        cost_estimate=cost,
        compiler_params=limit(50900),
        name="late",
    )(sums, states, earlier, *common)
    return exchange(sums + moved)[None]


def solution(mesh):
    return jax.shard_map(
        shards,
        mesh=mesh,
        in_specs=(
            P("groups", None, None),
            P(("groups", "steps", "inner"), None, None, None),
            P(("groups", "steps", "inner")),
            P("groups"),
            P(),
            P(),
            P(),
            P(),
            P(),
        ),
        out_specs=P(("groups", "steps", "inner"), None, None, None),
        check_vma=False,
    )
```

```python
import functools
import math

import jax
import jax.numpy as jnp
import numpy as np
from jax import lax
from jax.experimental import pallas as pl
from jax.experimental.pallas import tpu as pltpu
from jax.sharding import PartitionSpec as P

GROUPS = 32
TRAIN_STEPS = 1000
TIME = ("steps", "inner")
LANES = 128
CHUNK = 256
COEFS = 5
SPLIT = 1


def noise_table():
    levels = np.arange(TRAIN_STEPS, dtype=np.float64)
    betas = 0.0001 + (0.02 - 0.0001) * levels / (TRAIN_STEPS - 1)
    padded = np.zeros((1, -(-TRAIN_STEPS // LANES) * LANES), np.float32)
    padded[0, :TRAIN_STEPS] = np.exp(np.cumsum(np.log1p(-betas)))
    return padded


def group_mean(sums, size, count):
    lane = lax.broadcasted_iota(jnp.int32, sums.shape, 1)
    reach = 1
    while reach < size:
        upper = (lane & reach) != 0
        sums = sums + jnp.where(
            upper, pltpu.roll(sums, reach, 1), pltpu.roll(sums, LANES - reach, 1)
        )
        reach *= 2
    return sums * (1.0 / count)


def norm_silu(hidden_ref, act_ref, first, times, size, scale_ref, shift_ref):
    rows = hidden_ref.shape[0]
    patches = rows // times
    for lane in range(first, first + CHUNK, LANES):
        columns = slice(lane, lane + LANES)
        values = hidden_ref[:, columns].reshape(patches, times, LANES)
        mean = group_mean(jnp.sum(values, axis=0), size, patches * size)
        offset = values - mean
        spread = group_mean(jnp.sum(offset * offset, axis=0), size, patches * size)
        gain = 0.5 * lax.rsqrt(spread + 1e-05)
        if scale_ref is None:
            half = offset * gain
        else:
            gain = gain * (1.0 + scale_ref[:, columns])
            half = offset * gain + 0.5 * shift_ref[:, columns]
        act = half * jnp.tanh(half) + half
        act_ref[:, columns] = act.reshape(rows, LANES).astype(jnp.bfloat16)


def dot(left, right):
    return jnp.dot(left, right, preferred_element_type=jnp.float32)


def first_stage(times, rows_ref, scale_ref, shift_ref, input_weight, copies, next_copies, entry_ref, one_ref):
    features, channels = input_weight.shape
    flat = jnp.concatenate([rows_ref[block] for block in range(features // LANES)], axis=1)
    flat = flat.astype(jnp.bfloat16)
    wait_all(copies)
    for parts in next_copies:
        start_all(parts)
    for first in range(0, channels, CHUNK):
        columns = slice(first, first + CHUNK)
        entry_ref[:, columns] = dot(flat, input_weight[:, columns])
        norm_silu(entry_ref, one_ref, first, times, channels // GROUPS, scale_ref, shift_ref)


def later_stages(times, weights, copies, add_entry, hidden_ref, one_ref, two_ref, eps_ref):
    first_weight, second_weight, output_weight = weights
    channels, features = output_weight.shape
    size = channels // GROUPS
    wait_all(copies[0])
    for first in range(0, channels, CHUNK):
        columns = slice(first, first + CHUNK)
        hidden_ref[:, columns] = dot(one_ref[...], first_weight[:, columns])
        norm_silu(hidden_ref, two_ref, first, times, size, None, None)
    wait_all(copies[1])
    for first in range(0, channels, CHUNK):
        columns = slice(first, first + CHUNK)
        hidden_ref[:, columns] = add_entry(columns, dot(two_ref[...], second_weight[:, columns]))
        norm_silu(hidden_ref, one_ref, first, times, size, None, None)
    wait_all(copies[2])
    for first in range(0, features, CHUNK):
        part = dot(one_ref[...], output_weight[:, first : first + CHUNK])
        for lane in range(0, CHUNK, LANES):
            eps_ref[(first + lane) // LANES] = part[:, lane : lane + LANES]


def coefficients(now, later):
    ratio = (1.0 - later) / (1.0 - now)
    keep = ratio * jnp.sqrt(now / later)
    return (
        1.0 / jnp.sqrt(now),
        jnp.sqrt((1.0 - now) / now),
        (later - now) / (jnp.sqrt(later) * (1.0 - now)),
        keep - 1.0,
        jnp.sqrt(ratio * (1.0 - now / later)),
    )


def drift(state, eps, noise, coefs):
    inverse, slope, clean_part, state_part, sigma = coefs
    clean = jnp.clip(inverse * state - slope * eps, -1.0, 1.0)
    return clean_part * clean + state_part * state + sigma * noise


def plan_copies(sources, targets, sems):
    copies = []
    for index, (source, target) in enumerate(zip(sources, targets)):
        step = source.shape[0] // SPLIT
        parts = [
            pltpu.make_async_copy(
                source.at[pl.ds(part * step, step)],
                target.at[pl.ds(part * step, step)],
                sems.at[index * SPLIT + part],
            )
            for part in range(SPLIT)
        ]
        copies.append(parts)
    return copies


def start_all(parts):
    for part in parts:
        part.start()


def wait_all(parts):
    for part in parts:
        part.wait()


def spread_rows(rows_ref, step, stride, values):
    patches, features = values.shape
    for block in range(features // LANES):
        part = values[:, block * LANES : (block + 1) * LANES]
        rows_ref[block, pl.ds(step, patches, stride), :] = part


def prepare_kernel(
    width,
    start_hbm,
    input_hbm,
    gaps_ref,
    opening_ref,
    own_ref,
    entry_ref,
    norm_ref,
    part_ref,
    input_ref,
    own_sem,
    sems,
):
    place = lax.axis_index(TIME)
    own_copy = pltpu.make_async_copy(start_hbm.at[lax.rem(place, width)], own_ref, own_sem)
    own_copy.start()
    (copies,) = plan_copies((input_hbm,), (input_ref,), sems)
    start_all(copies)
    later = lax.broadcasted_iota(jnp.int32, part_ref.shape, 1) > place
    opening = jnp.where(place == 0, opening_ref[0], 0)
    part_ref[...] = opening - jnp.where(later, gaps_ref[0], 0)
    own_copy.wait()
    patches = own_ref.shape[0]
    channels = input_ref.shape[1]
    size = channels // GROUPS
    flat = own_ref[...].astype(jnp.bfloat16)
    wait_all(copies)
    for first in range(0, channels, CHUNK):
        columns = slice(first, first + CHUNK)
        entry_ref[:, columns] = dot(flat, input_ref[:, columns])
        for lane in range(first, first + CHUNK, LANES):
            columns = slice(lane, lane + LANES)
            values = entry_ref[:, columns]

            def mean(part):
                sums = jnp.sum(part, axis=0, keepdims=True)
                sums = jnp.broadcast_to(sums, (width, LANES))
                return group_mean(sums, size, patches * size)[:1]

            offset = values - mean(values)
            norm_ref[:, columns] = offset * lax.rsqrt(mean(offset * offset) + 1e-05)


def first_kernel(
    width,
    own_ref,
    entry_ref,
    norm_ref,
    noise_ref,
    marks_ref,
    table_ref,
    embed_hbm,
    first_hbm,
    second_hbm,
    output_hbm,
    state_ref,
    total_ref,
    scale_ref,
    shift_ref,
    coef_ref,
    hidden_ref,
    one_ref,
    two_ref,
    eps_ref,
    embed_ref,
    first_ref,
    second_ref,
    output_ref,
    sems,
):
    embed_copies, *copies = plan_copies(
        (embed_hbm, first_hbm, second_hbm, output_hbm),
        (embed_ref, first_ref, second_ref, output_ref),
        sems,
    )
    start_all(embed_copies)
    start_all(copies[0])
    place = lax.axis_index(TIME)
    image = lax.rem(place, width)
    patches, features = own_ref.shape
    lane = lax.broadcasted_iota(jnp.int32, (width, marks_ref.shape[1]), 1)
    time = lax.broadcasted_iota(jnp.int32, lane.shape, 0)
    marks = marks_ref[...].astype(jnp.float32)
    spot = place - image + time
    now_mark = jnp.sum(jnp.where(lane == spot, marks, 0.0), axis=1, keepdims=True)
    next_mark = jnp.sum(jnp.where(lane == spot + 1, marks, 0.0), axis=1, keepdims=True)
    level = lax.broadcasted_iota(jnp.int32, (width, table_ref.shape[1]), 1).astype(jnp.float32)
    table = table_ref[...]
    now = jnp.sum(jnp.where(level == now_mark, table, 0.0), axis=1, keepdims=True)
    later = jnp.sum(jnp.where(level == next_mark, table, 0.0), axis=1, keepdims=True)
    coefs = coefficients(now, later)
    for index, coef in enumerate(coefs):
        coef_ref[index] = jnp.broadcast_to(coef, (width, LANES))

    half = embed_ref.shape[0] // 2
    order = lax.broadcasted_iota(jnp.int32, (1, half), 1).astype(jnp.float32)
    angles = now_mark * jnp.exp(-math.log(10000.0) * order / half)
    channels = norm_ref.shape[1]
    cosine = jnp.cos(angles).astype(jnp.bfloat16)
    sine = jnp.sin(angles).astype(jnp.bfloat16)
    both = jnp.concatenate([cosine, sine], axis=1)
    wait_all(embed_copies)
    start_all(copies[1])
    start_all(copies[2])
    scale_ref[...] = dot(both, embed_ref[:, :channels])
    shift_ref[...] = dot(both, embed_ref[:, channels:])

    for lane in range(0, channels, LANES):
        columns = slice(lane, lane + LANES)
        gain = 0.5 * (1.0 + scale_ref[:, columns])
        lift = 0.5 * shift_ref[:, columns]
        half = norm_ref[:, columns][:, None, :] * gain[None] + lift[None]
        act = half * jnp.tanh(half) + half
        one_ref[:, columns] = act.reshape(patches * width, LANES).astype(jnp.bfloat16)

    def add_entry(columns, part):
        entry = entry_ref[:, columns]
        return (part.reshape(patches, width, -1) + entry[:, None, :]).reshape(part.shape)

    weights = (first_ref, second_ref, output_ref)
    later_stages(width, weights, copies, add_entry, hidden_ref, one_ref, two_ref, eps_ref)
    for block in range(features // LANES):
        columns = slice(block * LANES, (block + 1) * LANES)
        base = own_ref[:, columns]
        running = None
        for step in range(width):
            eps = eps_ref[block, pl.ds(step, patches, width), :]
            row = [coef_ref[index, step : step + 1, :] for index in range(COEFS)]
            state_ref[step, :, columns] = base if running is None else base + running
            change = drift(base, eps, noise_ref[step, :, columns], row)
            running = change if running is None else running + change
        total_ref[:, columns] = running


def early_kernel(width, *refs):
    @pl.when(lax.axis_index(TIME) < width)
    def _():
        second_kernel(width, refs[0], None, *refs[1:])


def late_kernel(width, sums_ref, *refs):
    @pl.when(lax.axis_index(TIME) >= width)
    def _():
        second_kernel(width, *refs[:11], None, *refs[11:])


def second_kernel(
    width,
    state_ref,
    earlier_ref,
    noise_ref,
    scale_ref,
    shift_ref,
    coef_ref,
    input_ref,
    first_hbm,
    second_hbm,
    output_hbm,
    sum_ref,
    total_ref,
    rows_ref,
    entry_ref,
    hidden_ref,
    one_ref,
    two_ref,
    eps_ref,
    first_ref,
    second_ref,
    output_ref,
    sems,
):
    weights = (first_ref, second_ref, output_ref)
    copies = plan_copies((first_hbm, second_hbm, output_hbm), weights, sems)
    for parts in copies:
        start_all(parts)
    _, patches, features = state_ref.shape

    def state_of(step, columns):
        state = state_ref[step, :, columns]
        return state if earlier_ref is None else state + earlier_ref[:, columns]

    for step in range(width):
        spread_rows(rows_ref, step, width, state_of(step, slice(None)))
    first_stage(
        width, rows_ref, scale_ref, shift_ref, input_ref, (), (), entry_ref, one_ref
    )

    def add_entry(columns, part):
        return entry_ref[:, columns] + part

    later_stages(width, weights, copies, add_entry, hidden_ref, one_ref, two_ref, eps_ref)
    for block in range(features // LANES):
        columns = slice(block * LANES, (block + 1) * LANES)
        own = state_ref[0, :, columns]
        running = None
        for step in range(width):
            eps = eps_ref[block, pl.ds(step, patches, width), :]
            row = [coef_ref[index, step : step + 1, :] for index in range(COEFS)]
            change = drift(state_of(step, columns), eps, noise_ref[step, :, columns], row)
            running = change if running is None else running + change
            sum_ref[step, :, columns] = own + running
        if total_ref is not None:
            total_ref[:, columns] = running


def shift_blocks(part, count, width, blocks):
    pairs = [(place, place + blocks * width) for place in range(count - blocks * width)]
    return lax.ppermute(part, TIME, pairs)


def earlier_blocks(part, count, width):
    total = shift_blocks(part, count, width, 1)
    reach = 1
    while reach < count // width - 1:
        total = total + shift_blocks(total, count, width, reach)
        reach *= 2
    return total


def shards(
    start_state,
    noise_draws,
    step_gaps,
    window_start,
    input_weight,
    embed_weight,
    first_weight,
    second_weight,
    output_weight,
):
    count = lax.axis_size(TIME)
    width, patches, features = start_state.shape
    channels = input_weight.shape[1]
    assert count % width == 0 and width % 8 == 0
    groups = [list(range(first, first + width)) for first in range(0, count, width)]
    def exchange(values):
        return lax.all_to_all(values, TIME, 0, 0, axis_index_groups=groups, tiled=True)

    noise = exchange(noise_draws[0])
    marks_length = -(-(count + 1) // LANES) * LANES

    def shape(*dims):
        return jax.ShapeDtypeStruct(dims, jnp.float32)

    vmem = pl.BlockSpec(memory_space=pltpu.VMEM)
    hbm = pl.BlockSpec(memory_space=pltpu.HBM)
    rows = width * patches
    blocked = pltpu.VMEM((features // LANES, rows, LANES), jnp.float32)
    wide = pltpu.VMEM((rows, channels), jnp.float32)
    act = pltpu.VMEM((rows, channels), jnp.bfloat16)

    def holder(weight):
        return pltpu.VMEM(weight.shape, weight.dtype)

    later = (first_weight, second_weight, output_weight)
    later_weights = [holder(weight) for weight in later]

    def limit(kib):
        return pltpu.CompilerParams(vmem_limit_bytes=kib * 1024)

    smem = pl.BlockSpec(memory_space=pltpu.SMEM)
    own, entry, norm, part = pl.pallas_call(
        functools.partial(prepare_kernel, width),
        out_shape=(
            shape(patches, features),
            shape(patches, channels),
            shape(patches, channels),
            jax.ShapeDtypeStruct((1, marks_length), jnp.int32),
        ),
        in_specs=[hbm] * 2 + [smem] * 2,
        out_specs=(vmem,) * 4,
        scratch_shapes=[
            holder(input_weight),
            pltpu.SemaphoreType.DMA,
            pltpu.SemaphoreType.DMA((SPLIT,)),
        ],
        compiler_params=limit(54800),
        name="prepare",
    )(start_state, input_weight, step_gaps, window_start)
    marks = lax.psum(part, TIME)
    states, total, scale, shift, coefs = pl.pallas_call(
        functools.partial(first_kernel, width),
        out_shape=(
            shape(width, patches, features),
            shape(patches, features),
            shape(width, channels),
            shape(width, channels),
            shape(COEFS, width, LANES),
        ),
        in_specs=[vmem] * 6 + [hbm] * 4,
        out_specs=(vmem,) * 5,
        scratch_shapes=[wide, act, act, blocked, holder(embed_weight), *later_weights]
        + [pltpu.SemaphoreType.DMA((4 * SPLIT,))],
        compiler_params=limit(51300),
        name="first",
    )(
        own,
        entry,
        norm,
        noise,
        marks,
        jnp.asarray(noise_table()),
        embed_weight,
        first_weight,
        second_weight,
        output_weight,
    )
    scratch = [blocked, wide, wide, act, act, blocked, *later_weights]
    scratch.append(pltpu.SemaphoreType.DMA((4 * SPLIT,)))
    sums_shape = shape(width, patches, features)
    total_shape = shape(patches, features)
    common = (noise, scale, shift, coefs, input_weight, *later)
    flops = 2 * rows * channels * (2 * features + 2 * channels)
    cost = pl.CostEstimate(flops=flops, transcendentals=0, bytes_accessed=8 * 2**20)
    if count != 2 * width:
        sums, total = pl.pallas_call(
            functools.partial(second_kernel, width),
            out_shape=(sums_shape, total_shape),
            in_specs=[vmem] * 7 + [hbm] * 3,
            out_specs=(vmem,) * 2,
            scratch_shapes=scratch,
            compiler_params=limit(50900),
            name="second",
        )(states, earlier_blocks(total, count, width), *common)
        return exchange(sums + earlier_blocks(total, count, width))[None]
    earlier = earlier_blocks(total, count, width)
    sums, total = pl.pallas_call(
        functools.partial(early_kernel, width),
        out_shape=(sums_shape, total_shape),
        in_specs=[vmem] * 6 + [hbm] * 3,
        out_specs=(vmem,) * 2,
        scratch_shapes=scratch,
        cost_estimate=cost,
        compiler_params=limit(50900),
        name="early",
    )(states, *common)
    moved = earlier_blocks(total, count, width)
    sums = pl.pallas_call(
        functools.partial(late_kernel, width),
        out_shape=sums_shape,
        in_specs=[vmem] * 8 + [hbm] * 3,
        out_specs=vmem,
        scratch_shapes=scratch,
        input_output_aliases={0: 0},
        cost_estimate=cost,
        compiler_params=limit(50900),
        name="late",
    )(sums, states, earlier, *common)
    return exchange(sums + moved)[None]


def solution(mesh):
    return jax.shard_map(
        shards,
        mesh=mesh,
        in_specs=(
            P("groups", None, None),
            P(("groups", "steps", "inner"), None, None, None),
            P(("groups", "steps", "inner")),
            P("groups"),
            P(),
            P(),
            P(),
            P(),
            P(),
        ),
        out_specs=P(("groups", "steps", "inner"), None, None, None),
        check_vma=False,
    )
```
